32 devices in a mesh: row: 4 (over x, core), col: 8 (over z, y).
Axes of the slice: x: 2, y: 2, z: 4, core: 2. Of those that a mesh axis runs over, the one named last changes fastest.
Arguments:
- picture_embedding_matrix: bfloat16 [2048, 1152], P(('row', 'col')), may hold values from -0.19921875 to 0.19921875
- caption_embedding_matrix: bfloat16 [2048, 1152], P(('row', 'col')), may hold values from -0.19921875 to 0.19921875
- sharpness_scale: float32 [1], replicated, may hold values from 4 to 12
- additive_shift: float32 [1], replicated, may hold values from -4 to -2
Outputs:
- grad_images: float32 [2048, 1152], P(('row', 'col'))
- grad_texts: float32 [2048, 1152], P(('row', 'col'))
- image_loss: float32 [2048], P(('row', 'col'))
The draws below stay inside these ranges and needn't reach their ends.
All inputs are finite; a program needn't handle non-finite values.
Results may differ from the reference program's by a relative error of at most 0.0053.
Values may be sent and summed in bfloat16 or wider, within the bound.
A program may use at most 128 MiB of HBM per device.

```python
import jax
import jax.numpy as jnp
from jax import lax

D = 1152
ROWS_DEV = 64
BATCH = 2048
N_COL = 8


def block_levels(rng, extent, pieces, least, high):
    level, own = 1.0, jax.random.fold_in(rng, 6)
    for position, shards_of in pieces:
        heights = jnp.exp(jax.random.uniform(jax.random.fold_in(own, position), (shards_of,), jnp.float32, least / len(pieces), high / len(pieces)))
        level = level * jnp.repeat(heights, extent[position] // shards_of).reshape([-1 if axis == position else 1 for axis in range(len(extent))])
    return level


def scatter_about(rng, extent, spread, most, split=(), kind=jnp.bfloat16):
    entries = spread * jax.random.normal(rng, extent, jnp.float32)
    if split:
        entries = entries * block_levels(rng, extent, split, -0.22, 0.18)
    return jnp.clip(entries, -most, most).astype(kind)


def setup_inputs(seed: int = 0) -> dict:
    splits = jax.random.split(jax.random.key(seed), 5)
    return {
        "picture_embedding_matrix": scatter_about(splits[0], (BATCH, D), 0.03, 0.19921875, ((0, 32),)),
        "caption_embedding_matrix": scatter_about(splits[1], (BATCH, D), 0.03, 0.19921875, ((0, 32),)),
        "sharpness_scale": jnp.clip(jax.random.uniform(splits[2], (1,), jnp.float32, 4.0, 12.0), 4.0, 12.0),
        "additive_shift": jnp.clip(jax.random.uniform(splits[3], (1,), jnp.float32, -4.0, -2.0), -4.0, -2.0),
    }


EPS = 1e-06

def normalize(feats):
    values = feats.astype(jnp.float32)
    inverse = lax.rsqrt(lax.optimization_barrier(jnp.sum(values * values, axis=-1, keepdims=True)) + EPS)
    return (values * inverse, inverse)

def back_norm(grad, unit, inverse):
    return inverse * (grad - unit * lax.optimization_barrier(jnp.sum(unit * grad, axis=-1, keepdims=True)))

def reference(picture_embedding_matrix, caption_embedding_matrix, sharpness_scale, additive_shift):
    img_f, img_inv = normalize(picture_embedding_matrix)
    txt_f, txt_inv = normalize(caption_embedding_matrix)
    img_b = img_f.astype(jnp.bfloat16)
    caption_segment = txt_f.astype(jnp.bfloat16)
    block = ROWS_DEV * N_COL
    blocks = BATCH // block
    columns = jnp.arange(BATCH, dtype=jnp.int32)

    def step(acc, index):
        start = (index * block).astype(jnp.int32)
        sample_total = lax.dynamic_slice_in_dim(img_b, start, block, 0)
        similarity_matrix = jnp.dot(sample_total, caption_segment.T, preferred_element_type=jnp.float32) * sharpness_scale[0] + additive_shift[0]
        ids = start + jnp.arange(block, dtype=jnp.int32)
        match_sign = ids[:, None] == columns[None, :]
        label = jnp.where(match_sign, jnp.float32(1.0), jnp.float32(-1.0))
        sigmoid_loss = lax.optimization_barrier(jnp.sum(jnp.log1p(jnp.exp(-label * similarity_matrix)), axis=1))
        logistic_weight = (sharpness_scale[0] * (jax.nn.sigmoid(similarity_matrix) - match_sign.astype(jnp.float32))).astype(jnp.bfloat16)
        g_rows = jnp.dot(logistic_weight, caption_segment, preferred_element_type=jnp.float32)
        acc = acc + lax.dot_general(logistic_weight, sample_total, (((0,), (0,)), ((), ())), preferred_element_type=jnp.float32)
        return (acc, (g_rows, sigmoid_loss))
    start_acc = jnp.zeros((BATCH, D), jnp.float32)
    g_txt, (g_img, sigmoid_loss) = lax.scan(step, start_acc, jnp.arange(blocks, dtype=jnp.int32))
    g_img = g_img.reshape(BATCH, D)
    sigmoid_loss = sigmoid_loss.reshape(BATCH)
    return (back_norm(g_img, img_f, img_inv), back_norm(g_txt, txt_f, txt_inv), sigmoid_loss)
```

```python
import functools

import jax
import jax.numpy as jnp
from jax import lax
from jax.experimental import pallas as pl
from jax.experimental.pallas import tpu as pltpu
from jax.sharding import PartitionSpec as P

EPS = 1e-06
MESH = pl.DeviceIdType.MESH
PIECES = 2
TILE = 256


def bits_of(n):
    return n.bit_length() - 1


def groups(n_row, n_col):
    row_bits, col_bits = bits_of(n_row), bits_of(n_col)
    take = min(max((row_bits + col_bits + 1) // 2 - row_bits, 0), col_bits)
    choice = [b for b in range(1, col_bits)] + [0] * (col_bits > 0)
    mine, rest = choice[:take], choice[take:]
    images = [("col", b) for b in sorted(mine, reverse=True)]
    images += [("row", b) for b in reversed(range(row_bits))]
    texts = [("col", b) for b in sorted(rest, reverse=True)]
    return images, texts


def flip(index, bit):
    step = 2**bit
    return index + step * (1 - 2 * lax.rem(lax.div(index, step), 2))


def peer_of(dims, mask):
    at = {"row": lax.axis_index("row"), "col": lax.axis_index("col")}
    for j, (axis, bit) in enumerate(dims):
        if mask >> j & 1:
            at[axis] = flip(at[axis], bit)
    return (at["row"], at["col"])


def top(slot):
    return slot.bit_length() - 1


def inverse_norm(values):
    return lax.rsqrt(jnp.sum(values * values, axis=-1, keepdims=True) + EPS)


def tiles(count, body):
    if count <= 4:
        for t in range(count):
            body(t)
    else:
        lax.fori_loop(0, count, lambda t, _: (body(t), 0)[1], 0)


def kernel(
    dims,
    own_img,
    own_txt,
    scale_ref,
    shift_ref,
    gi_ref,
    gt_ref,
    loss_ref,
    img_raw,
    txt_raw,
    img_n,
    txt_n,
    coef,
    acc_img,
    acc_txt,
    out_img,
    out_txt,
    in_img,
    in_txt,
    loss_sum,
    loss_out,
    loss_in,
    gs_img,
    gr_img,
    gs_txt,
    gr_txt,
    ss_img,
    sr_img,
    ss_txt,
    sr_txt,
    ls,
    lr,
):
    rows, _ = own_img.shape
    part = rows // PIECES
    size = {"i": 2 ** len(dims["i"]), "t": 2 ** len(dims["t"])}
    own = {"i": own_img, "t": own_txt}
    raw = {"i": img_raw, "t": txt_raw}
    unit = {"i": img_n, "t": txt_n}
    acc = {"i": acc_img, "t": acc_txt}
    out = {"i": out_img, "t": out_txt}
    into = {"i": in_img, "t": in_txt}
    g_sems = {"i": (gs_img, gr_img), "t": (gs_txt, gr_txt)}
    s_sems = {"i": (ss_img, sr_img), "t": (ss_txt, sr_txt)}
    sent = []

    peers = [peer_of(dims["i"], m) for m in range(1, size["i"])]
    peers += [peer_of(dims["t"], 2**j) for j in range(len(dims["t"]))]
    barrier = pltpu.get_barrier_semaphore()
    for peer in peers:
        pl.semaphore_signal(barrier, inc=1, device_id=peer, device_id_type=MESH)
    pl.semaphore_wait(barrier, len(peers))

    gather = {}

    def spread(g, slot, j, p):
        to = slot | 1 << j
        piece = pl.ds(p * part, part)
        source = own[g].at[piece] if slot == 0 else raw[g].at[slot, piece]
        copy = pltpu.make_async_remote_copy(
            src_ref=source,
            dst_ref=raw[g].at[to, piece],
            send_sem=g_sems[g][0].at[to, p],
            recv_sem=g_sems[g][1].at[to, p],
            device_id=peer_of(dims[g], 1 << j),
            device_id_type=MESH,
        )
        copy.start()
        gather[g, to, p] = copy
        sent.append(copy)

    for p in range(PIECES):
        for j in range(max(len(dims["i"]), len(dims["t"]))):
            for g in ("t", "i"):
                if j < len(dims[g]):
                    spread(g, 0, j, p)

    def normalize(g, slot):
        values = (own[g][...] if slot == 0 else raw[g][slot]).astype(jnp.float32)
        unit[g][slot * rows : (slot + 1) * rows, :] = (values * inverse_norm(values)).astype(
            jnp.bfloat16
        )

    normalize("i", 0)
    normalize("t", 0)
    levels = max(len(dims["i"]), len(dims["t"]))
    for level in range(1, levels + 1):
        slots = [
            (g, s)
            for s in reversed(range(1, max(size.values())))
            for g in ("i", "t")
            if s < size[g] and s.bit_count() == level
        ]
        for p in range(PIECES):
            for g, s in slots:
                gather[g, s, p].wait_recv()
                for j in range(top(s) + 1, len(dims[g])):
                    spread(g, s, j, p)
                if p == PIECES - 1:
                    normalize(g, s)

    scale, shift = scale_ref[0], shift_ref[0]
    n_img, n_txt = size["i"] * rows, size["t"] * rows
    t_img, t_txt = min(TILE, n_img), min(TILE, n_txt)
    loss_sum[...] = jnp.zeros_like(loss_sum)

    def logits(t):
        if isinstance(t, int):
            at_txt, at_img = t // (n_img // t_img) * t_txt, t % (n_img // t_img) * t_img
        else:
            at_txt = pl.multiple_of(lax.div(t, n_img // t_img) * t_txt, t_txt)
            at_img = pl.multiple_of(lax.rem(t, n_img // t_img) * t_img, t_img)
        here_txt, here_img = pl.ds(at_txt, t_txt), pl.ds(at_img, t_img)
        value = lax.dot_general(
            txt_n[here_txt, :],
            img_n[here_img, :],
            (((1,), (1,)), ((), ())),
            preferred_element_type=jnp.float32,
        )
        value = value * scale + shift
        weight = scale
        if not isinstance(t, int) or t == 0:
            a = lax.broadcasted_iota(jnp.int32, value.shape, 0) + at_txt
            b = lax.broadcasted_iota(jnp.int32, value.shape, 1) + at_img
            match = (a == b) & (a < rows)
            value = jnp.where(match, -value, value)
            weight = jnp.where(match, -scale, scale)
        e = jnp.exp(value)
        loss_sum[:, here_img] += jnp.sum(jnp.log1p(e), axis=0, keepdims=True)
        coef[here_txt, here_img] = (weight * (e / (1.0 + e))).astype(jnp.bfloat16)

    tiles((n_txt // t_txt) * (n_img // t_img), logits)

    losses = []
    for s in range(1, size["i"]):
        loss_out[s] = loss_sum[:, s * rows : (s + 1) * rows]
        copy = pltpu.make_async_remote_copy(
            src_ref=loss_out.at[s],
            dst_ref=loss_in.at[s],
            send_sem=ls.at[s],
            recv_sem=lr.at[s],
            device_id=peer_of(dims["i"], s),
            device_id_type=MESH,
        )
        copy.start()
        losses.append(copy)
        sent.append(copy)

    scatter = {}

    def pass_on(g, s, p):
        piece = pl.ds(p * part, part)
        copy = pltpu.make_async_remote_copy(
            src_ref=out[g].at[s, piece],
            dst_ref=into[g].at[s, piece],
            send_sem=s_sems[g][0].at[s, p],
            recv_sem=s_sems[g][1].at[s, p],
            device_id=peer_of(dims[g], 1 << top(s)),
            device_id_type=MESH,
        )
        copy.start()
        scatter[g, s, p] = copy
        sent.append(copy)

    def product(g, first, count):
        here = pl.ds(first * rows, count * rows)
        if not isinstance(first, int):
            here = pl.ds(pl.multiple_of(first * rows, count * rows), count * rows)
        if g == "t":
            return jnp.dot(coef[here, :], img_n[...], preferred_element_type=jnp.float32)
        return lax.dot_general(
            coef[:, here], txt_n[...], (((0,), (0,)), ((), ())), preferred_element_type=jnp.float32
        )

    def grads(g, upper):
        half = size[g] // 2
        base = half if upper else 0
        step = min(half, TILE // rows)

        def body(t):
            first = base + t * step
            value = product(g, first, step)
            if upper:
                out[g][pl.ds(first, step)] = value.reshape(step, rows, -1).astype(jnp.bfloat16)
            else:
                acc[g][pl.ds(first, step)] = value.reshape(step, rows, -1)

        tiles(half // step, body)
        if upper:
            for s in reversed(range(half, size[g])):
                for p in range(PIECES):
                    pass_on(g, s, p)

    grads("t", True)
    grads("i", True)
    grads("i", False)
    grads("t", False)

    def total(g, k, p):
        piece = pl.ds(p * part, part)
        value = acc[g][k, piece]
        for j in reversed(range(top(k) + 1 if k else 0, len(dims[g]))):
            scatter[g, k | 1 << j, p].wait_recv()
            value = value + into[g][k | 1 << j, piece].astype(jnp.float32)
        return value

    order = sorted(
        [(k.bit_length() - len(dims[g]), g, k) for g in ("i", "t") for k in range(1, size[g] // 2)],
        key=lambda item: (-item[0], item[1] != "i", -item[2]),
    )
    for _, g, k in order:
        for p in range(PIECES):
            out[g][k, pl.ds(p * part, part)] = total(g, k, p).astype(jnp.bfloat16)
            pass_on(g, k, p)

    value = loss_sum[:, :rows]
    for s, copy in enumerate(losses, 1):
        copy.wait_recv()
        value = value + loss_in[s]
    loss_ref[...] = value

    for g, result in (("i", gi_ref), ("t", gt_ref)):
        for p in range(PIECES):
            piece = pl.ds(p * part, part)
            grad = total(g, 0, p)
            values = own[g][piece].astype(jnp.float32)
            inverse = inverse_norm(values)
            unit_row = values * inverse
            along = jnp.sum(unit_row * grad, axis=-1, keepdims=True)
            result[piece, :] = inverse * (grad - unit_row * along)

    for copy in sent:
        copy.wait_send()


def on_device(n_row, n_col, images, texts, scale, shift):
    rows, width = images.shape
    dims = dict(zip("it", groups(n_row, n_col)))
    a, b = 2 ** len(dims["i"]), 2 ** len(dims["t"])
    vmem = pl.BlockSpec(memory_space=pltpu.VMEM)
    smem = pl.BlockSpec(memory_space=pltpu.SMEM)
    f32, bf16 = jnp.float32, jnp.bfloat16
    gi, gt, loss = pl.pallas_call(
        functools.partial(kernel, dims),
        out_shape=(
            jax.ShapeDtypeStruct((rows, width), f32),
            jax.ShapeDtypeStruct((rows, width), f32),
            jax.ShapeDtypeStruct((1, rows), f32),
        ),
        in_specs=[vmem, vmem, smem, smem],
        out_specs=(vmem, vmem, vmem),
        scratch_shapes=[
            pltpu.VMEM((a, rows, width), bf16),
            pltpu.VMEM((b, rows, width), bf16),
            pltpu.VMEM((a * rows, width), bf16),
            pltpu.VMEM((b * rows, width), bf16),
            pltpu.VMEM((b * rows, a * rows), bf16),
            pltpu.VMEM((a // 2, rows, width), f32),
            pltpu.VMEM((b // 2, rows, width), f32),
            pltpu.VMEM((a, rows, width), bf16),
            pltpu.VMEM((b, rows, width), bf16),
            pltpu.VMEM((a, rows, width), bf16),
            pltpu.VMEM((b, rows, width), bf16),
            pltpu.VMEM((1, a * rows), f32),
            pltpu.VMEM((a, 1, rows), f32),
            pltpu.VMEM((a, 1, rows), f32),
        ]
        + [pltpu.SemaphoreType.DMA((n, PIECES)) for n in (a, a, b, b, a, a, b, b)]
        + [pltpu.SemaphoreType.DMA((a,)), pltpu.SemaphoreType.DMA((a,))],
        compiler_params=pltpu.CompilerParams(collective_id=0, has_side_effects=True),
    )(images, texts, scale, shift)
    return gi, gt, loss.reshape(rows)


def solution(mesh):
    placed = (P(("row", "col"), None), P(("row", "col"), None), P(), P())
    return jax.shard_map(
        functools.partial(on_device, mesh.shape["row"], mesh.shape["col"]),
        mesh=mesh,
        in_specs=placed,
        out_specs=(P(("row", "col"), None), P(("row", "col"), None), P(("row", "col"))),
        check_vma=False,
    )
```

```python
import functools

import jax
import jax.numpy as jnp
from jax import lax
from jax.experimental import pallas as pl
from jax.experimental.pallas import tpu as pltpu
from jax.sharding import PartitionSpec as P

EPS = 1e-06
MESH = pl.DeviceIdType.MESH
PIECES = 2
TILE = 256


def bits_of(n):
    return n.bit_length() - 1


def groups(n_row, n_col):
    row_bits, col_bits = bits_of(n_row), bits_of(n_col)
    take = min(max((row_bits + col_bits + 1) // 2 - row_bits, 0), col_bits)
    choice = [b for b in range(1, col_bits)] + [0] * (col_bits > 0)
    mine, rest = choice[:take], choice[take:]
    images = [("col", b) for b in sorted(mine, reverse=True)]
    images += [("row", b) for b in reversed(range(row_bits))]
    texts = [("col", b) for b in sorted(rest, reverse=True)]
    return images, texts


def flip(index, bit):
    step = 2**bit
    return index + step * (1 - 2 * lax.rem(lax.div(index, step), 2))


def peer_of(dims, mask):
    at = {"row": lax.axis_index("row"), "col": lax.axis_index("col")}
    for j, (axis, bit) in enumerate(dims):
        if mask >> j & 1:
            at[axis] = flip(at[axis], bit)
    return (at["row"], at["col"])


def top(slot):
    return slot.bit_length() - 1


def inverse_norm(values):
    return lax.rsqrt(jnp.sum(values * values, axis=-1, keepdims=True) + EPS)


def tiles(count, body):
    if count <= 4:
        for t in range(count):
            body(t)
    else:
        lax.fori_loop(0, count, lambda t, _: (body(t), 0)[1], 0)


def kernel(
    dims,
    img_hbm,
    txt_hbm,
    scale_ref,
    shift_ref,
    gi_ref,
    gt_ref,
    loss_ref,
    own_img,
    own_txt,
    load,
    img_raw,
    txt_raw,
    img_n,
    txt_n,
    coef,
    acc_img,
    acc_txt,
    out_img,
    out_txt,
    in_img,
    in_txt,
    loss_sum,
    loss_out,
    loss_in,
    gs_img,
    gr_img,
    gs_txt,
    gr_txt,
    ss_img,
    sr_img,
    ss_txt,
    sr_txt,
    ls,
    lr,
):
    rows, _ = img_hbm.shape
    part = rows // PIECES
    size = {"i": 2 ** len(dims["i"]), "t": 2 ** len(dims["t"])}
    own = {"i": own_img, "t": own_txt}
    raw = {"i": img_raw, "t": txt_raw}
    unit = {"i": img_n, "t": txt_n}
    acc = {"i": acc_img, "t": acc_txt}
    out = {"i": out_img, "t": out_txt}
    into = {"i": in_img, "t": in_txt}
    g_sems = {"i": (gs_img, gr_img), "t": (gs_txt, gr_txt)}
    s_sems = {"i": (ss_img, sr_img), "t": (ss_txt, sr_txt)}
    sent = []

    peers = [peer_of(dims["i"], m) for m in range(1, size["i"])]
    peers += [peer_of(dims["t"], 2**j) for j in range(len(dims["t"]))]
    barrier = pltpu.get_barrier_semaphore()
    for peer in peers:
        pl.semaphore_signal(barrier, inc=1, device_id=peer, device_id_type=MESH)
    loads = [
        pltpu.make_async_copy(source, target, load.at[n])
        for n, (source, target) in enumerate(
            [
                (txt_hbm, own_txt),
                (img_hbm, own_img),
            ]
        )
    ]
    for copy in loads:
        copy.start()
    for copy in loads:
        copy.wait()
    pl.semaphore_wait(barrier, len(peers))

    gather = {}

    def spread(g, slot, j, p):
        to = slot | 1 << j
        piece = pl.ds(p * part, part)
        source = own[g].at[piece] if slot == 0 else raw[g].at[slot, piece]
        copy = pltpu.make_async_remote_copy(
            src_ref=source,
            dst_ref=raw[g].at[to, piece],
            send_sem=g_sems[g][0].at[to, p],
            recv_sem=g_sems[g][1].at[to, p],
            device_id=peer_of(dims[g], 1 << j),
            device_id_type=MESH,
        )
        copy.start()
        gather[g, to, p] = copy
        sent.append(copy)

    for p in range(PIECES):
        for j in range(max(len(dims["i"]), len(dims["t"]))):
            for g in ("i", "t"):
                if j < len(dims[g]):
                    spread(g, 0, j, p)

    def normalize(g, slot):
        values = (own[g][...] if slot == 0 else raw[g][slot]).astype(jnp.float32)
        unit[g][slot * rows : (slot + 1) * rows, :] = (values * inverse_norm(values)).astype(
            jnp.bfloat16
        )

    normalize("i", 0)
    normalize("t", 0)
    levels = max(len(dims["i"]), len(dims["t"]))
    for level in range(1, levels + 1):
        slots = [
            (g, s)
            for s in reversed(range(1, max(size.values())))
            for g in ("i", "t")
            if s < size[g] and s.bit_count() == level
        ]
        for p in range(PIECES):
            for g, s in slots:
                gather[g, s, p].wait_recv()
                for j in range(top(s) + 1, len(dims[g])):
                    spread(g, s, j, p)
                if p == PIECES - 1:
                    normalize(g, s)

    scale, shift = scale_ref[0], shift_ref[0]
    n_img, n_txt = size["i"] * rows, size["t"] * rows
    t_img, t_txt = min(TILE, n_img), min(TILE, n_txt)
    loss_sum[...] = jnp.zeros_like(loss_sum)

    def logits(t):
        if isinstance(t, int):
            at_txt, at_img = t // (n_img // t_img) * t_txt, t % (n_img // t_img) * t_img
        else:
            at_txt = pl.multiple_of(lax.div(t, n_img // t_img) * t_txt, t_txt)
            at_img = pl.multiple_of(lax.rem(t, n_img // t_img) * t_img, t_img)
        here_txt, here_img = pl.ds(at_txt, t_txt), pl.ds(at_img, t_img)
        value = lax.dot_general(
            txt_n[here_txt, :],
            img_n[here_img, :],
            (((1,), (1,)), ((), ())),
            preferred_element_type=jnp.float32,
        )
        value = value * scale + shift
        weight = scale
        if not isinstance(t, int) or t == 0:
            a = lax.broadcasted_iota(jnp.int32, value.shape, 0) + at_txt
            b = lax.broadcasted_iota(jnp.int32, value.shape, 1) + at_img
            match = (a == b) & (a < rows)
            value = jnp.where(match, -value, value)
            weight = jnp.where(match, -scale, scale)
        e = jnp.exp(value)
        loss_sum[:, here_img] += jnp.sum(jnp.log1p(e), axis=0, keepdims=True)
        coef[here_txt, here_img] = (weight * (e / (1.0 + e))).astype(jnp.bfloat16)

    tiles((n_txt // t_txt) * (n_img // t_img), logits)

    losses = []
    for s in range(1, size["i"]):
        loss_out[s] = loss_sum[:, s * rows : (s + 1) * rows]
        copy = pltpu.make_async_remote_copy(
            src_ref=loss_out.at[s],
            dst_ref=loss_in.at[s],
            send_sem=ls.at[s],
            recv_sem=lr.at[s],
            device_id=peer_of(dims["i"], s),
            device_id_type=MESH,
        )
        copy.start()
        losses.append(copy)
        sent.append(copy)

    scatter = {}

    def pass_on(g, s, p):
        piece = pl.ds(p * part, part)
        copy = pltpu.make_async_remote_copy(
            src_ref=out[g].at[s, piece],
            dst_ref=into[g].at[s, piece],
            send_sem=s_sems[g][0].at[s, p],
            recv_sem=s_sems[g][1].at[s, p],
            device_id=peer_of(dims[g], 1 << top(s)),
            device_id_type=MESH,
        )
        copy.start()
        scatter[g, s, p] = copy
        sent.append(copy)

    def product(g, first, count):
        here = pl.ds(first * rows, count * rows)
        if not isinstance(first, int):
            here = pl.ds(pl.multiple_of(first * rows, count * rows), count * rows)
        if g == "t":
            return jnp.dot(coef[here, :], img_n[...], preferred_element_type=jnp.float32)
        return lax.dot_general(
            coef[:, here], txt_n[...], (((0,), (0,)), ((), ())), preferred_element_type=jnp.float32
        )

    def grads(g, upper):
        half = size[g] // 2
        base = half if upper else 0
        step = min(half, TILE // rows)

        def body(t):
            first = base + t * step
            value = product(g, first, step)
            if upper:
                out[g][pl.ds(first, step)] = value.reshape(step, rows, -1).astype(jnp.bfloat16)
            else:
                acc[g][pl.ds(first, step)] = value.reshape(step, rows, -1)

        tiles(half // step, body)
        if upper:
            for s in reversed(range(half, size[g])):
                for p in range(PIECES):
                    pass_on(g, s, p)

    grads("t", True)
    grads("i", True)
    grads("i", False)
    grads("t", False)

    def total(g, k, p):
        piece = pl.ds(p * part, part)
        value = acc[g][k, piece]
        for j in reversed(range(top(k) + 1 if k else 0, len(dims[g]))):
            scatter[g, k | 1 << j, p].wait_recv()
            value = value + into[g][k | 1 << j, piece].astype(jnp.float32)
        return value

    order = sorted(
        [(k.bit_length() - len(dims[g]), g, k) for g in ("i", "t") for k in range(1, size[g] // 2)],
        key=lambda item: (-item[0], item[1] != "i", -item[2]),
    )
    for _, g, k in order:
        for p in range(PIECES):
            out[g][k, pl.ds(p * part, part)] = total(g, k, p).astype(jnp.bfloat16)
            pass_on(g, k, p)

    value = loss_sum[:, :rows]
    for s, copy in enumerate(losses, 1):
        copy.wait_recv()
        value = value + loss_in[s]
    loss_ref[...] = value

    for g, result in (("i", gi_ref), ("t", gt_ref)):
        for p in range(PIECES):
            piece = pl.ds(p * part, part)
            grad = total(g, 0, p)
            values = own[g][piece].astype(jnp.float32)
            inverse = inverse_norm(values)
            unit_row = values * inverse
            along = jnp.sum(unit_row * grad, axis=-1, keepdims=True)
            result[piece, :] = inverse * (grad - unit_row * along)

    for copy in sent:
        copy.wait_send()


def hand_out(gi_from, gt_from, loss_from, gi_ref, gt_ref, loss_ref, sems):
    pairs = ((gi_from, gi_ref), (gt_from, gt_ref), (loss_from, loss_ref))
    copies = [pltpu.make_async_copy(a, b, sems.at[n]) for n, (a, b) in enumerate(pairs)]
    for copy in copies:
        copy.start()
    for copy in copies:
        copy.wait()


def on_device(n_row, n_col, images, texts, scale, shift):
    rows, width = images.shape
    dims = dict(zip("it", groups(n_row, n_col)))
    a, b = 2 ** len(dims["i"]), 2 ** len(dims["t"])
    vmem = pl.BlockSpec(memory_space=pltpu.VMEM)
    smem = pl.BlockSpec(memory_space=pltpu.SMEM)
    hbm = pl.BlockSpec(memory_space=pl.ANY)
    f32, bf16 = jnp.float32, jnp.bfloat16
    sums = pl.pallas_call(
        functools.partial(kernel, dims),
        out_shape=(
            pltpu.VMEM((rows, width), f32),
            pltpu.VMEM((rows, width), f32),
            pltpu.VMEM((1, rows), f32),
        ),
        in_specs=[hbm, hbm, smem, smem],
        out_specs=(vmem, vmem, vmem),
        scratch_shapes=[
            pltpu.VMEM((rows, width), bf16),
            pltpu.VMEM((rows, width), bf16),
            pltpu.SemaphoreType.DMA((2,)),
            pltpu.VMEM((a, rows, width), bf16),
            pltpu.VMEM((b, rows, width), bf16),
            pltpu.VMEM((a * rows, width), bf16),
            pltpu.VMEM((b * rows, width), bf16),
            pltpu.VMEM((b * rows, a * rows), bf16),
            pltpu.VMEM((a // 2, rows, width), f32),
            pltpu.VMEM((b // 2, rows, width), f32),
            pltpu.VMEM((a, rows, width), bf16),
            pltpu.VMEM((b, rows, width), bf16),
            pltpu.VMEM((a, rows, width), bf16),
            pltpu.VMEM((b, rows, width), bf16),
            pltpu.VMEM((1, a * rows), f32),
            pltpu.VMEM((a, 1, rows), f32),
            pltpu.VMEM((a, 1, rows), f32),
        ]
        + [pltpu.SemaphoreType.DMA((n, PIECES)) for n in (a, a, b, b, a, a, b, b)]
        + [pltpu.SemaphoreType.DMA((a,)), pltpu.SemaphoreType.DMA((a,))],
        compiler_params=pltpu.CompilerParams(collective_id=0, has_side_effects=True),
    )(*[pltpu.with_memory_space_constraint(x, pltpu.HBM) for x in (images, texts)], scale, shift)
    gi, gt, loss = pl.pallas_call(
        hand_out,
        out_shape=(
            jax.ShapeDtypeStruct((rows, width), f32),
            jax.ShapeDtypeStruct((rows, width), f32),
            jax.ShapeDtypeStruct((1, rows), f32),
        ),
        in_specs=[hbm] * 3,
        out_specs=(hbm, hbm, hbm),
        scratch_shapes=[pltpu.SemaphoreType.DMA((3,))],
    )(*[pltpu.with_memory_space_constraint(x, pltpu.VMEM) for x in sums])
    return gi, gt, loss.reshape(rows)


def solution(mesh):
    placed = (P(("row", "col"), None), P(("row", "col"), None), P(), P())
    return jax.shard_map(
        functools.partial(on_device, mesh.shape["row"], mesh.shape["col"]),
        mesh=mesh,
        in_specs=placed,
        out_specs=(P(("row", "col"), None), P(("row", "col"), None), P(("row", "col"))),
        check_vma=False,
    )
```

```python
import functools

import jax
import jax.numpy as jnp
from jax import lax
from jax.experimental import pallas as pl
from jax.experimental.pallas import tpu as pltpu
from jax.sharding import PartitionSpec as P

EPS = 1e-06
MESH = pl.DeviceIdType.MESH
PIECES = 2
TILE = 256


def bits_of(n):
    return n.bit_length() - 1


def groups(n_row, n_col):
    row_bits, col_bits = bits_of(n_row), bits_of(n_col)
    take = min(max((row_bits + col_bits + 1) // 2 - row_bits, 0), col_bits)
    choice = [b for b in range(1, col_bits)] + [0] * (col_bits > 0)
    mine, rest = choice[:take], choice[take:]
    images = [("col", b) for b in sorted(mine, reverse=True)]
    images += [("row", b) for b in reversed(range(row_bits))]
    texts = [("col", b) for b in sorted(rest, reverse=True)]
    return images, texts


def flip(index, bit):
    step = 2**bit
    return index + step * (1 - 2 * lax.rem(lax.div(index, step), 2))


def peer_of(dims, mask):
    at = {"row": lax.axis_index("row"), "col": lax.axis_index("col")}
    for j, (axis, bit) in enumerate(dims):
        if mask >> j & 1:
            at[axis] = flip(at[axis], bit)
    return (at["row"], at["col"])


def top(slot):
    return slot.bit_length() - 1


def inverse_norm(values):
    return lax.rsqrt(jnp.sum(values * values, axis=-1, keepdims=True) + EPS)


def tiles(count, body):
    if count <= 4:
        for t in range(count):
            body(t)
    else:
        lax.fori_loop(0, count, lambda t, _: (body(t), 0)[1], 0)


def kernel(
    dims,
    img_hbm,
    txt_hbm,
    scale_ref,
    shift_ref,
    gi_ref,
    gt_ref,
    loss_ref,
    own_img,
    own_txt,
    load,
    img_raw,
    txt_raw,
    img_n,
    txt_n,
    coef,
    acc_img,
    acc_txt,
    out_img,
    out_txt,
    in_img,
    in_txt,
    loss_sum,
    loss_out,
    loss_in,
    gs_img,
    gr_img,
    gs_txt,
    gr_txt,
    ss_img,
    sr_img,
    ss_txt,
    sr_txt,
    ls,
    lr,
):
    rows, _ = img_hbm.shape
    part = rows // PIECES
    size = {"i": 2 ** len(dims["i"]), "t": 2 ** len(dims["t"])}
    own = {"i": own_img, "t": own_txt}
    raw = {"i": img_raw, "t": txt_raw}
    unit = {"i": img_n, "t": txt_n}
    acc = {"i": acc_img, "t": acc_txt}
    out = {"i": out_img, "t": out_txt}
    into = {"i": in_img, "t": in_txt}
    g_sems = {"i": (gs_img, gr_img), "t": (gs_txt, gr_txt)}
    s_sems = {"i": (ss_img, sr_img), "t": (ss_txt, sr_txt)}
    sent = []

    peers = [peer_of(dims["i"], m) for m in range(1, size["i"])]
    peers += [peer_of(dims["t"], 2**j) for j in range(len(dims["t"]))]
    barrier = pltpu.get_barrier_semaphore()
    for peer in peers:
        pl.semaphore_signal(barrier, inc=1, device_id=peer, device_id_type=MESH)
    loads = [
        pltpu.make_async_copy(source, target, load.at[n])
        for n, (source, target) in enumerate(
            [
                (txt_hbm, own_txt),
                (img_hbm, own_img),
            ]
        )
    ]
    for copy in loads:
        copy.start()
    for copy in loads:
        copy.wait()
    pl.semaphore_wait(barrier, len(peers))

    gather = {}

    def spread(g, slot, j, p):
        to = slot | 1 << j
        piece = pl.ds(p * part, part)
        source = own[g].at[piece] if slot == 0 else raw[g].at[slot, piece]
        copy = pltpu.make_async_remote_copy(
            src_ref=source,
            dst_ref=raw[g].at[to, piece],
            send_sem=g_sems[g][0].at[to, p],
            recv_sem=g_sems[g][1].at[to, p],
            device_id=peer_of(dims[g], 1 << j),
            device_id_type=MESH,
        )
        copy.start()
        gather[g, to, p] = copy
        sent.append(copy)

    for p in range(PIECES):
        for j in range(max(len(dims["i"]), len(dims["t"]))):
            for g in ("i", "t"):
                if j < len(dims[g]):
                    spread(g, 0, j, p)

    def normalize(g, slot):
        values = (own[g][...] if slot == 0 else raw[g][slot]).astype(jnp.float32)
        unit[g][slot * rows : (slot + 1) * rows, :] = (values * inverse_norm(values)).astype(
            jnp.bfloat16
        )

    normalize("i", 0)
    normalize("t", 0)
    levels = max(len(dims["i"]), len(dims["t"]))
    for level in range(1, levels + 1):
        slots = [
            (g, s)
            for s in reversed(range(1, max(size.values())))
            for g in ("i", "t")
            if s < size[g] and s.bit_count() == level
        ]
        for p in range(PIECES):
            for g, s in slots:
                gather[g, s, p].wait_recv()
                for j in range(top(s) + 1, len(dims[g])):
                    spread(g, s, j, p)
                if p == PIECES - 1:
                    normalize(g, s)

    scale, shift = scale_ref[0], shift_ref[0]
    n_img, n_txt = size["i"] * rows, size["t"] * rows
    t_img, t_txt = min(TILE, n_img), min(TILE, n_txt)
    loss_sum[...] = jnp.zeros_like(loss_sum)

    def logits(t):
        if isinstance(t, int):
            at_txt, at_img = t // (n_img // t_img) * t_txt, t % (n_img // t_img) * t_img
        else:
            at_txt = pl.multiple_of(lax.div(t, n_img // t_img) * t_txt, t_txt)
            at_img = pl.multiple_of(lax.rem(t, n_img // t_img) * t_img, t_img)
        here_txt, here_img = pl.ds(at_txt, t_txt), pl.ds(at_img, t_img)
        value = lax.dot_general(
            txt_n[here_txt, :],
            img_n[here_img, :],
            (((1,), (1,)), ((), ())),
            preferred_element_type=jnp.float32,
        )
        value = value * scale + shift
        weight = scale
        if not isinstance(t, int) or t == 0:
            a = lax.broadcasted_iota(jnp.int32, value.shape, 0) + at_txt
            b = lax.broadcasted_iota(jnp.int32, value.shape, 1) + at_img
            match = (a == b) & (a < rows)
            value = jnp.where(match, -value, value)
            weight = jnp.where(match, -scale, scale)
        e = jnp.exp(value)
        loss_sum[:, here_img] += jnp.sum(jnp.log1p(e), axis=0, keepdims=True)
        coef[here_txt, here_img] = (weight * (e / (1.0 + e))).astype(jnp.bfloat16)

    tiles((n_txt // t_txt) * (n_img // t_img), logits)

    losses = []
    for s in range(1, size["i"]):
        loss_out[s] = loss_sum[:, s * rows : (s + 1) * rows]
        copy = pltpu.make_async_remote_copy(
            src_ref=loss_out.at[s],
            dst_ref=loss_in.at[s],
            send_sem=ls.at[s],
            recv_sem=lr.at[s],
            device_id=peer_of(dims["i"], s),
            device_id_type=MESH,
        )
        copy.start()
        losses.append(copy)
        sent.append(copy)

    scatter = {}

    def pass_on(g, s, p):
        piece = pl.ds(p * part, part)
        copy = pltpu.make_async_remote_copy(
            src_ref=out[g].at[s, piece],
            dst_ref=into[g].at[s, piece],
            send_sem=s_sems[g][0].at[s, p],
            recv_sem=s_sems[g][1].at[s, p],
            device_id=peer_of(dims[g], 1 << top(s)),
            device_id_type=MESH,
        )
        copy.start()
        scatter[g, s, p] = copy
        sent.append(copy)

    def product(g, first, count):
        here = pl.ds(first * rows, count * rows)
        if not isinstance(first, int):
            here = pl.ds(pl.multiple_of(first * rows, count * rows), count * rows)
        if g == "t":
            return jnp.dot(coef[here, :], img_n[...], preferred_element_type=jnp.float32)
        return lax.dot_general(
            coef[:, here], txt_n[...], (((0,), (0,)), ((), ())), preferred_element_type=jnp.float32
        )

    def grads(g, upper):
        half = size[g] // 2
        base = half if upper else 0
        step = min(half, TILE // rows)

        def body(t):
            first = base + t * step
            value = product(g, first, step)
            if upper:
                out[g][pl.ds(first, step)] = value.reshape(step, rows, -1).astype(jnp.bfloat16)
            else:
                acc[g][pl.ds(first, step)] = value.reshape(step, rows, -1)

        tiles(half // step, body)
        if upper:
            for s in reversed(range(half, size[g])):
                for p in range(PIECES):
                    pass_on(g, s, p)

    grads("t", True)
    grads("i", True)
    grads("i", False)
    grads("t", False)

    def total(g, k, p):
        piece = pl.ds(p * part, part)
        value = acc[g][k, piece]
        for j in reversed(range(top(k) + 1 if k else 0, len(dims[g]))):
            scatter[g, k | 1 << j, p].wait_recv()
            value = value + into[g][k | 1 << j, piece].astype(jnp.float32)
        return value

    order = sorted(
        [(k.bit_length() - len(dims[g]), g, k) for g in ("i", "t") for k in range(1, size[g] // 2)],
        key=lambda item: (-item[0], item[1] != "i", -item[2]),
    )
    for _, g, k in order:
        for p in range(PIECES):
            out[g][k, pl.ds(p * part, part)] = total(g, k, p).astype(jnp.bfloat16)
            pass_on(g, k, p)

    for g, result in (("i", gi_ref), ("t", gt_ref)):
        for p in range(PIECES):
            piece = pl.ds(p * part, part)
            grad = total(g, 0, p)
            values = own[g][piece].astype(jnp.float32)
            inverse = inverse_norm(values)
            unit_row = values * inverse
            along = jnp.sum(unit_row * grad, axis=-1, keepdims=True)
            result[piece, :] = inverse * (grad - unit_row * along)

    value = loss_sum[:, :rows]
    for s, copy in enumerate(losses, 1):
        copy.wait_recv()
        value = value + loss_in[s]
    loss_ref[...] = value

    for copy in sent:
        copy.wait_send()


def hand_out(gi_from, gt_from, loss_from, gi_ref, gt_ref, loss_ref, sems):
    pairs = ((gi_from, gi_ref), (gt_from, gt_ref), (loss_from, loss_ref))
    copies = [pltpu.make_async_copy(a, b, sems.at[n]) for n, (a, b) in enumerate(pairs)]
    for copy in copies:
        copy.start()
    for copy in copies:
        copy.wait()


def on_device(n_row, n_col, images, texts, scale, shift):
    rows, width = images.shape
    dims = dict(zip("it", groups(n_row, n_col)))
    a, b = 2 ** len(dims["i"]), 2 ** len(dims["t"])
    vmem = pl.BlockSpec(memory_space=pltpu.VMEM)
    smem = pl.BlockSpec(memory_space=pltpu.SMEM)
    hbm = pl.BlockSpec(memory_space=pl.ANY)
    f32, bf16 = jnp.float32, jnp.bfloat16
    sums = pl.pallas_call(
        functools.partial(kernel, dims),
        out_shape=(
            pltpu.VMEM((rows, width), f32),
            pltpu.VMEM((rows, width), f32),
            pltpu.VMEM((1, rows), f32),
        ),
        in_specs=[hbm, hbm, smem, smem],
        out_specs=(vmem, vmem, vmem),
        scratch_shapes=[
            pltpu.VMEM((rows, width), bf16),
            pltpu.VMEM((rows, width), bf16),
            pltpu.SemaphoreType.DMA((2,)),
            pltpu.VMEM((a, rows, width), bf16),
            pltpu.VMEM((b, rows, width), bf16),
            pltpu.VMEM((a * rows, width), bf16),
            pltpu.VMEM((b * rows, width), bf16),
            pltpu.VMEM((b * rows, a * rows), bf16),
            pltpu.VMEM((a // 2, rows, width), f32),
            pltpu.VMEM((b // 2, rows, width), f32),
            pltpu.VMEM((a, rows, width), bf16),
            pltpu.VMEM((b, rows, width), bf16),
            pltpu.VMEM((a, rows, width), bf16),
            pltpu.VMEM((b, rows, width), bf16),
            pltpu.VMEM((1, a * rows), f32),
            pltpu.VMEM((a, 1, rows), f32),
            pltpu.VMEM((a, 1, rows), f32),
        ]
        + [pltpu.SemaphoreType.DMA((n, PIECES)) for n in (a, a, b, b, a, a, b, b)]
        + [pltpu.SemaphoreType.DMA((a,)), pltpu.SemaphoreType.DMA((a,))],
        compiler_params=pltpu.CompilerParams(collective_id=0, has_side_effects=True),
    )(*[pltpu.with_memory_space_constraint(x, pltpu.HBM) for x in (images, texts)], scale, shift)
    gi, gt, loss = pl.pallas_call(
        hand_out,
        out_shape=(
            jax.ShapeDtypeStruct((rows, width), f32),
            jax.ShapeDtypeStruct((rows, width), f32),
            jax.ShapeDtypeStruct((1, rows), f32),
        ),
        in_specs=[hbm] * 3,
        out_specs=(hbm, hbm, hbm),
        scratch_shapes=[pltpu.SemaphoreType.DMA((3,))],
    )(*[pltpu.with_memory_space_constraint(x, pltpu.VMEM) for x in sums])
    return gi, gt, loss.reshape(rows)


def solution(mesh):
    placed = (P(("row", "col"), None), P(("row", "col"), None), P(), P())
    return jax.shard_map(
        functools.partial(on_device, mesh.shape["row"], mesh.shape["col"]),
        mesh=mesh,
        in_specs=placed,
        out_specs=(P(("row", "col"), None), P(("row", "col"), None), P(("row", "col"))),
        check_vma=False,
    )
```
